32 devices in a mesh: row: 4 (over x, core), col: 4 (over z), tp: 2 (over y).
Axes of the slice: x: 2, y: 2, z: 4, core: 2. Of those that a mesh axis runs over, the one named last changes fastest.
Arguments:
- tokens: bfloat16 [8192, 1024], P(('row', 'col'), 'tp'), may hold values from -6 to 6
- norm_before: bfloat16 [2, 1024], replicated, may hold values from 0.099609375 to 1.8984375
- query_weight: bfloat16 [2, 1024, 1024], P(None, None, 'tp'), may hold values from -0.1875 to 0.1875
- key_weight: bfloat16 [2, 1024, 1024], P(None, None, 'tp'), may hold values from -8 to 8
- value_weight: bfloat16 [2, 1024, 1024], P(None, None, 'tp'), may hold values from -0.1875 to 0.1875
- output_weight: bfloat16 [2, 1024, 1024], P(None, 'tp'), may hold values from -0.375 to 0.375
- norm_after: bfloat16 [2, 1024], replicated, may hold values from 0.099609375 to 1.8984375
- gate_weight: bfloat16 [2, 1024, 4096], P(None, None, 'tp'), may hold values from -0.1875 to 0.1875
- up_weight: bfloat16 [2, 1024, 4096], P(None, None, 'tp'), may hold values from -0.1875 to 0.1875
- down_weight: bfloat16 [2, 4096, 1024], P(None, 'tp'), may hold values from -0.09375 to 0.09375
- block_image: int32 [64], replicated, may hold values from 0 to 3, never falling along the last dimension, each value on 1 to 29 neighbouring positions
- image_width: int32 [4], replicated, may hold values from 16 to 64
Outputs:
- encoded: float32 [8192, 1024], P(('row', 'col'), 'tp')
The draws below stay inside these ranges and needn't reach their ends.
Inputs may be any that keep to these rules, and one draw needn't show every extreme that they name: `block_image`: image numbers never fall from block to block; each image fills 1 to 29 whole blocks of 128 patch slots, and one image fills exactly 29.
All inputs are finite; a program needn't handle non-finite values.
Results may differ from the reference program's by a relative error of at most 0.035.
The reference program's roundings to bfloat16 on the way count: a program that leaves them out, or rounds other values in their place, can miss the bound.
Values may be sent and summed in bfloat16 or wider, within the bound.
No kernel may reach another device: no remote copies, remote signals or barrier semaphores. Data moves between devices by JAX's collectives and lax.ppermute only.
A program may use at most 128 MiB of HBM per device.

```python
import math
import jax
import jax.numpy as jnp
import numpy as np
from jax import lax

D = 1024
HEADS = 16
FF = 4096
HEAD_DIM = 64
BLK = 128
LAYERS = 2
BLOCKS = 64
TOKENS = 8192
IMAGES = 4
MOST_BLK = 29


def draw_tokens(key, part):
    base = jnp.clip(jax.random.normal(jax.random.fold_in(key, 11), (TOKENS, D), jnp.float32), -6.0, 6.0)
    return base.astype(jnp.bfloat16)


def draw_key_weight(key, part):
    base = jnp.clip(jax.random.normal(jax.random.fold_in(key, 21), (LAYERS, D, D), jnp.float32), -4.0, 4.0) * D ** (-0.5)
    return base.astype(jnp.bfloat16)


def plant(values, stream_key, low, top_value):
    shape = values.shape
    index_at = [jax.random.randint(jax.random.fold_in(stream_key, axis), (), 0, shape[axis]) for axis in range(len(shape))]
    values = values.at[tuple(index_at)].set(low)
    longest = shape.index(max(shape))
    index_at[longest] = (index_at[longest] + 1) % shape[longest]
    return values.at[tuple(index_at)].set(top_value)


def level_of(rng, extent, cuts, low, high):
    def one(position, shards_of):
        steps = jax.random.uniform(jax.random.fold_in(jax.random.fold_in(rng, 6), position), (shards_of,), jnp.float32, low / len(cuts), high / len(cuts))
        return jnp.repeat(jnp.exp(steps), extent[position] // shards_of).reshape((-1,) + (1,) * (len(extent) - position - 1))

    level = one(*cuts[0])
    for cut in cuts[1:]:
        level = level * one(*cut)
    return level


def split_up(amount, total, most, lean):
    loads = [(1 << 20) // math.isqrt(standing ** lean) + 1 for standing in range(2, amount + 1)]
    surplus, holding = total - most - (amount - 1), [1] * (amount - 1)
    while surplus > 0:
        movable = [i for i in range(amount - 1) if holding[i] < most]
        whole, budget = sum([loads[i] for i in movable]), surplus
        for i in movable:
            extra = min(most - holding[i], max(1, budget * loads[i] // whole), surplus)
            holding[i] = holding[i] + extra
            surplus = surplus - extra
    return np.array([most] + holding)


def uneven_parts(rng, amount, total, limit, slope):
    if amount == 2:
        one = jax.random.randint(rng, (), max(1, total - limit), min(limit, total - 1) + 1)
        return jnp.stack([one, total - one])
    tallies = jnp.asarray(split_up(amount, total, limit, slope), jnp.int32)
    twos = (amount - 1) // 2
    source_of, taker = tallies[1:1 + 2 * twos:2], tallies[2:2 + 2 * twos:2]
    room = jnp.minimum(source_of - 1, limit - taker)
    moved = jax.random.randint(jax.random.fold_in(rng, 1), (twos,), 0, 1 << 20) % (room + 1)
    tallies = tallies.at[1:1 + 2 * twos:2].set(source_of - moved).at[2:2 + 2 * twos:2].set(taker + moved)
    return tallies[jax.random.permutation(jax.random.fold_in(rng, 2), amount)]


def centred(stream_key, shape, scale, reach, shards=(), held_as=jnp.bfloat16):
    array = jax.random.normal(stream_key, shape, jnp.float32) * scale
    if len(shards) > 0:
        array = level_of(stream_key, shape, shards, -0.22, 0.18) * array
    return jnp.clip(array, min=-reach, max=reach).astype(held_as)


def setup_inputs(seed: int = 0) -> dict:
    key_list = jax.random.split(jax.random.key(seed), 13)
    tokens = draw_tokens(jax.random.fold_in(key_list[12], 71), 0)
    norm_before = jnp.clip(1.0 + 0.18 * jax.random.normal(key_list[1], (LAYERS, D), jnp.float32), 0.099609375, 1.8984375).astype(jnp.bfloat16)
    query_weight = centred(key_list[2], (LAYERS, D, D), D ** -0.5, 0.1875, ((2, 2),))
    key_weight = draw_key_weight(jax.random.fold_in(key_list[12], 71), 0)
    value_weight = centred(key_list[4], (LAYERS, D, D), D ** -0.5, 0.1875, ((2, 2),))
    output_weight = centred(key_list[5], (LAYERS, D, D), (4 * HEAD_DIM) ** -0.5, 0.375, ((1, 2),))
    norm_after = jnp.clip(1.0 + 0.18 * jax.random.normal(key_list[6], (LAYERS, D), jnp.float32), 0.099609375, 1.8984375).astype(jnp.bfloat16)
    gate_weight = centred(key_list[7], (LAYERS, D, FF), D ** -0.5, 0.1875, ((2, 2),))
    up_weight = centred(key_list[8], (LAYERS, D, FF), D ** -0.5, 0.1875, ((2, 2),))
    down_weight = centred(key_list[9], (LAYERS, FF, D), FF ** -0.5, 0.09375, ((1, 2),))
    block_image = jnp.searchsorted(jnp.cumsum(uneven_parts(key_list[10], IMAGES, BLOCKS, MOST_BLK, 2)), jnp.arange(BLOCKS), side="right").astype(jnp.int32)
    image_width = plant(jax.random.randint(key_list[11], (IMAGES,), BLK // 8, BLK // 2 + 1), jax.random.fold_in(key_list[11], 1), BLK // 8, (BLK // 2 + 1) - 1).astype(jnp.int32)
    return dict(tokens=tokens, norm_before=norm_before, query_weight=query_weight, key_weight=key_weight, value_weight=value_weight, output_weight=output_weight, norm_after=norm_after, gate_weight=gate_weight, up_weight=up_weight, down_weight=down_weight, block_image=block_image, image_width=image_width)


epsilon = 1e-05
theta = 10000.0
masked = -1e+30

def block_tables(block_image, image_width):
    block_total = block_image.shape[0]
    images = jnp.arange(image_width.shape[0], dtype=jnp.int32)
    member = (block_image[:, None] == images[None, :]).astype(jnp.int32)
    count = lax.optimization_barrier(jnp.sum(member, axis=0))
    start = lax.optimization_barrier(jnp.sum((block_image[:, None] < images[None, :]).astype(jnp.int32), axis=0))
    slots = count * BLK
    width = image_width.astype(jnp.int32)
    filled = slots // width * width
    first = lax.optimization_barrier(jnp.sum(member * start[None, :], axis=1))
    offset = (jnp.arange(block_total, dtype=jnp.int32) - first) * BLK
    return (block_image, offset, lax.optimization_barrier(jnp.sum(member * width[None, :], axis=1)), lax.optimization_barrier(jnp.sum(member * filled[None, :], axis=1)))

def token_rows(tables, first_block, shard_blocks):
    image, offset, width, filled = [jnp.repeat(lax.dynamic_slice_in_dim(table, first_block, shard_blocks), BLK) for table in tables]
    slot = offset + jnp.arange(shard_blocks * BLK, dtype=jnp.int32) % BLK
    return (image, slot // width, slot % width, slot < filled)

def rope_tables(patch_row, patch_column):
    half = HEAD_DIM // 2
    frequency = theta ** (-2.0 * jnp.arange(half, dtype=jnp.float32) / HEAD_DIM)
    angle = jnp.concatenate([patch_row.astype(jnp.float32)[:, None] * frequency[None, 0::2], patch_column.astype(jnp.float32)[:, None] * frequency[None, 1::2]], axis=1)
    return (jnp.cos(angle), jnp.sin(angle))

def rotate(heads, cosine, sine):
    half = heads.shape[-1] // 2
    front = heads[..., :half]
    back = heads[..., half:]
    cosine = cosine[:, None, :]
    sine = sine[:, None, :]
    return jnp.concatenate([front * cosine - back * sine, back * cosine + front * sine], axis=-1)

def normalize(values, gain):
    wide = values.astype(jnp.float32)
    scale = lax.rsqrt(lax.optimization_barrier(jnp.mean(wide * wide, axis=-1, keepdims=True)) + epsilon)
    return (wide * scale * gain.astype(jnp.float32)).astype(jnp.bfloat16)

def attention(query, keys, values, image, tags):
    rows = query.shape[0]
    block = math.gcd(rows, 256)
    margin = MOST_BLK * BLK
    length = min(rows, block + 2 * margin)
    scale = HEAD_DIM ** (-0.5)

    def one_block(index):
        begin = index * block
        key_start = jnp.clip(begin - margin, 0, rows - length)
        part_query = lax.dynamic_slice_in_dim(query, begin, block, 0).astype(jnp.float32)
        part_keys = lax.dynamic_slice_in_dim(keys, key_start, length, 0).astype(jnp.float32)
        part_values = lax.dynamic_slice_in_dim(values, key_start, length, 0).astype(jnp.float32)
        part_image = lax.dynamic_slice_in_dim(image, begin, block, 0)
        part_tags = lax.dynamic_slice_in_dim(tags, key_start, length, 0)
        scores = jnp.einsum('thd,uhd->thu', part_query, part_keys, precision=lax.Precision.HIGHEST) * scale
        allowed = (part_image[:, None] == part_tags[None, :])[:, None, :]
        top = lax.optimization_barrier(jnp.max(jnp.where(allowed, scores, masked), axis=-1, keepdims=True))
        raised = jnp.where(allowed, jnp.exp(scores - top), 0.0)
        total = lax.optimization_barrier(jnp.sum(raised, axis=-1))
        weights = lax.optimization_barrier(raised.astype(jnp.bfloat16)).astype(jnp.float32)
        summed = jnp.einsum('thu,uhd->thd', weights, part_values, precision=lax.Precision.HIGHEST)
        return (summed / total[..., None]).astype(jnp.bfloat16).reshape(block, -1)
    pieces = lax.map(one_block, jnp.arange(rows // block, dtype=jnp.int32))
    return pieces.reshape(rows, -1)

def reference(tokens, norm_before, query_weight, key_weight, value_weight, output_weight, norm_after, gate_weight, up_weight, down_weight, block_image, image_width):
    tables = block_tables(block_image, image_width)
    image, patch_row, patch_column, live = token_rows(tables, 0, block_image.shape[0])
    tags = jnp.where(live, image, -1)
    cosine, sine = rope_tables(patch_row, patch_column)
    rows = tokens.shape[0]
    hidden_state = tokens.astype(jnp.float32)
    for layer in range(LAYERS):
        normed = normalize(hidden_state, norm_before[layer])
        query = rotate(jnp.dot(normed, query_weight[layer], preferred_element_type=jnp.float32).reshape(rows, HEADS, HEAD_DIM), cosine, sine)
        query = lax.optimization_barrier(query.astype(jnp.bfloat16))
        keys = rotate(jnp.dot(normed, key_weight[layer], preferred_element_type=jnp.float32).reshape(rows, HEADS, HEAD_DIM), cosine, sine)
        keys = lax.optimization_barrier(keys.astype(jnp.bfloat16))
        values = jnp.dot(normed, value_weight[layer], preferred_element_type=jnp.float32).astype(jnp.bfloat16)
        values = lax.optimization_barrier(values).reshape(rows, HEADS, HEAD_DIM)
        attended = attention(query, keys, values, image, tags)
        middle = hidden_state + jnp.dot(attended, output_weight[layer], preferred_element_type=jnp.float32)
        post = normalize(middle, norm_after[layer])
        gate = jnp.dot(post, gate_weight[layer], preferred_element_type=jnp.float32)
        up = jnp.dot(post, up_weight[layer], preferred_element_type=jnp.float32)
        hidden = (jax.nn.silu(gate) * up).astype(jnp.bfloat16)
        hidden_state = middle + jnp.dot(hidden, down_weight[layer], preferred_element_type=jnp.float32)
    return hidden_state
```

```python
import functools

import jax
import jax.numpy as jnp
from jax import lax
from jax.experimental import pallas as pl
from jax.experimental.pallas import tpu as pltpu
from jax.sharding import PartitionSpec as P

HEAD_DIM = 64
BLK = 128
SPAN = 32

epsilon = 1e-05
theta = 10000.0
masked = -1e30


def block_tables(block_image, image_width):
    block_total = block_image.shape[0]
    images = jnp.arange(image_width.shape[0], dtype=jnp.int32)
    member = (block_image[:, None] == images[None, :]).astype(jnp.int32)
    count = jnp.sum(member, axis=0)
    start = jnp.sum((block_image[:, None] < images[None, :]).astype(jnp.int32), axis=0)
    slots = count * BLK
    filled = slots // image_width * image_width
    first = jnp.sum(member * start[None, :], axis=1)
    offset = (jnp.arange(block_total, dtype=jnp.int32) - first) * BLK
    return (
        block_image,
        offset,
        jnp.sum(member * image_width[None, :], axis=1),
        jnp.sum(member * filled[None, :], axis=1),
        first,
        first + jnp.sum(member * count[None, :], axis=1),
    )


def rope_transposed(tables, first_block, shard_blocks):
    offset, width = [
        lax.dynamic_slice_in_dim(tables[at], first_block, shard_blocks) for at in (1, 2)
    ]
    slot = offset[:, None] + jnp.arange(BLK, dtype=jnp.int32)[None, :]
    row = (slot // width[:, None]).reshape(1, -1).astype(jnp.float32)
    column = (slot % width[:, None]).reshape(1, -1).astype(jnp.float32)
    half = HEAD_DIM // 2
    frequency = theta ** (-2.0 * jnp.arange(half, dtype=jnp.float32) / HEAD_DIM)
    angle = jnp.concatenate([frequency[0::2, None] * row, frequency[1::2, None] * column], axis=0)
    return jnp.cos(angle), jnp.sin(angle)


def project_kernel(
    first, chips, place_ref, a_ref, b_ref, gain_ref, wq_ref, wk_ref, wv_ref, cos_ref, sin_ref, *refs
):
    whole_ref, pieces = refs[0], refs[1 : 1 + chips]
    staged = refs[1 + chips]
    chip, side = place_ref[0], place_ref[2]
    if first:
        own, other = a_ref[...].astype(jnp.float32), b_ref[...].astype(jnp.float32)
        whole = jnp.where(
            side == 0,
            jnp.concatenate([own, other], axis=1),
            jnp.concatenate([other, own], axis=1),
        )
    else:
        whole = a_ref[...] + b_ref[...].astype(jnp.float32)
    whole_ref[...] = whole
    scale = lax.rsqrt(jnp.mean(whole * whole, axis=1, keepdims=True) + epsilon)
    normed = (whole * scale * gain_ref[...].astype(jnp.float32)).astype(jnp.bfloat16)
    rows = whole.shape[0]
    half = HEAD_DIM // 2
    cosine, sine = cos_ref[...][None], sin_ref[...][None]
    for at, weight in enumerate((wq_ref, wk_ref, wv_ref)):
        result = jnp.dot(normed, weight[...], preferred_element_type=jnp.float32).T
        heads = result.shape[0] // HEAD_DIM
        result = result.reshape(heads, HEAD_DIM, rows)
        if at < 2:
            front, back = result[:, :half], result[:, half:]
            result = jnp.concatenate(
                [front * cosine - back * sine, back * cosine + front * sine], axis=1
            )
        if at == 0:
            result = result * (HEAD_DIM ** (-0.5) * 1.4426950408889634)
        staged[at] = result.astype(jnp.bfloat16)
    for step in range(chips):
        head = chip ^ step
        for at in range(3):
            pieces[step][at] = staged[at, head]


def project(first, chips, layer, place, a, b, gain, wq, wk, wv, cosine, sine):
    rows = a.shape[0]
    width = wq.shape[1]
    mine = wq.shape[2]
    whole_spec = lambda shape: pl.BlockSpec(shape, lambda i, p: (0,) * len(shape))
    weight_spec = pl.BlockSpec((None, width, mine), lambda i, p: (layer, 0, 0))
    results = pl.pallas_call(
        functools.partial(project_kernel, first, chips),
        grid_spec=pltpu.PrefetchScalarGridSpec(
            num_scalar_prefetch=1,
            grid=(1,),
            in_specs=[
                whole_spec(a.shape),
                whole_spec(b.shape),
                whole_spec((1, width)),
                weight_spec,
                weight_spec,
                weight_spec,
                whole_spec(cosine.shape),
                whole_spec(sine.shape),
            ],
            out_specs=[whole_spec((rows, width))] + [whole_spec((3, HEAD_DIM, rows))] * chips,
            scratch_shapes=[pltpu.VMEM((3, mine // HEAD_DIM, HEAD_DIM, rows), jnp.bfloat16)],
        ),
        out_shape=[jax.ShapeDtypeStruct((rows, width), jnp.float32)]
        + [jax.ShapeDtypeStruct((3, HEAD_DIM, rows), jnp.bfloat16)] * chips,
        compiler_params=pltpu.CompilerParams(vmem_limit_bytes=60 * 1024 * 1024),
        name="project",
    )(place, a, b, gain[layer][None], wq, wk, wv, cosine, sine)
    return results[0], list(results[1:])


ONES = 16
TILE = 256
KEYS = 512


def attend_kernel(chips, columns, table_ref, place_ref, *refs):
    own, other = refs[:chips], refs[chips : 2 * chips]
    outs = refs[2 * chips : 3 * chips]
    keys_s, values_s, query_s, result_s = refs[3 * chips :]
    chip, core = place_ref[0], place_ref[1]
    rows = own[0].shape[-1]
    blocks = rows // BLK
    total = keys_s.shape[0] - KEYS
    feature = lax.broadcasted_iota(jnp.int32, (HEAD_DIM, BLK), 0)
    lane = lax.broadcasted_iota(jnp.int32, (HEAD_DIM, BLK), 1)

    def place_of(step, side):
        at = chip ^ step
        return ((at // columns) * 2 + side) * columns + at % columns

    values_s[HEAD_DIM:, :] = jnp.ones((ONES, total + KEYS), jnp.bfloat16)
    values_s[:HEAD_DIM, total:] = jnp.zeros((HEAD_DIM, KEYS), jnp.bfloat16)
    keys_s[total:, :] = jnp.ones((KEYS, 2 * HEAD_DIM), jnp.bfloat16)
    for step in range(chips):
        for ref, first, side in ((own[step], 1, core), (other[step], 0, 1 - core)):
            place = place_of(step, side)
            base = pl.multiple_of(place * rows, BLK)
            barred = []
            for block in range(blocks):
                image = table_ref[0, place * blocks + block]
                live = table_ref[3, place * blocks + block]
                barred.append(
                    jnp.where((feature == image) & (lane < live), 0.0, 1.0)
                )
            extended = jnp.concatenate(
                [ref[first].astype(jnp.float32), jnp.concatenate(barred, axis=1)], axis=0
            )
            keys_s[pl.ds(base, rows), :] = extended.T.astype(jnp.bfloat16)
            values_s[:HEAD_DIM, pl.ds(base, rows)] = ref[first + 1]
        for part in range(rows // TILE):
            query_s[step, part] = own[step][0, :, part * TILE : (part + 1) * TILE]

    parts = rows // TILE
    tile_blocks = TILE // BLK

    def one_tile(index, unused):
        step, part = index // parts, index % parts
        first_block = place_of(step, core) * blocks + part * tile_blocks
        wanted = jnp.concatenate(
            [
                jnp.where(feature == table_ref[0, first_block + b], masked, 0.0)
                for b in range(tile_blocks)
            ],
            axis=1,
        ).astype(jnp.bfloat16)
        query = jnp.concatenate([query_s[step, part], wanted], axis=0)
        low = table_ref[1, first_block]
        high = table_ref[2, first_block + tile_blocks - 1]

        def visit(at, state):
            best, summed = state
            base = pl.multiple_of((low + at * (KEYS // BLK)) * BLK, BLK)
            scores = jnp.dot(
                keys_s[pl.ds(base, KEYS), :], query, preferred_element_type=jnp.float32
            )
            fresh = jnp.maximum(best, jnp.max(scores, axis=0, keepdims=True))
            raised = jnp.exp2(scores - fresh).astype(jnp.bfloat16)
            summed = summed * jnp.exp2(best - fresh) + jnp.dot(
                values_s[:, pl.ds(base, KEYS)], raised, preferred_element_type=jnp.float32
            )
            return fresh, summed

        visits = (high - low + (KEYS // BLK - 1)) // (KEYS // BLK)
        best, summed = lax.fori_loop(
            0,
            visits,
            visit,
            (
                jnp.full((1, TILE), masked, jnp.float32),
                jnp.zeros((HEAD_DIM + ONES, TILE), jnp.float32),
            ),
        )
        result_s[step, part] = (summed[:HEAD_DIM] / summed[HEAD_DIM : HEAD_DIM + 1]).astype(
            jnp.bfloat16
        )
        return unused

    lax.fori_loop(0, chips * parts, one_tile, 0)
    for step in range(chips):
        for part in range(parts):
            outs[step][:, part * TILE : (part + 1) * TILE] = result_s[step, part]


def attend(chips, columns, table, place, own, other):
    rows = own[0].shape[-1]
    total = table.shape[1] * BLK
    spec = lambda shape: pl.BlockSpec(shape, lambda i, t, p: (0,) * len(shape))
    return pl.pallas_call(
        functools.partial(attend_kernel, chips, columns),
        grid_spec=pltpu.PrefetchScalarGridSpec(
            num_scalar_prefetch=2,
            grid=(1,),
            in_specs=[spec(own[0].shape)] * chips + [spec(other[0].shape)] * chips,
            out_specs=[spec((HEAD_DIM, rows))] * chips,
            scratch_shapes=[
                pltpu.VMEM((total + KEYS, 2 * HEAD_DIM), jnp.bfloat16),
                pltpu.VMEM((HEAD_DIM + ONES, total + KEYS), jnp.bfloat16),
                pltpu.VMEM((chips, rows // TILE, HEAD_DIM, TILE), jnp.bfloat16),
                pltpu.VMEM((chips, rows // TILE, HEAD_DIM, TILE), jnp.bfloat16),
            ],
        ),
        out_shape=[jax.ShapeDtypeStruct((HEAD_DIM, rows), jnp.bfloat16)] * chips,
        compiler_params=pltpu.CompilerParams(vmem_limit_bytes=60 * 1024 * 1024),
        name="attend",
    )(table, place, *own, *other)


def feed_kernel(
    last, chips, steps, place_ref, whole_ref, gain_ref, wo_ref, wx_ref, wg_ref, wu_ref, wd_ref, *refs
):
    own, other = refs[:chips], refs[chips : 2 * chips]
    kept_ref, sent_ref = refs[2 * chips], refs[2 * chips + 1]
    middle_s, post_s, sum_s, own_s, other_s = refs[2 * chips + 2 :]
    chip, side = place_ref[0], place_ref[2]
    index = pl.program_id(0)

    @pl.when(index == 0)
    def _():
        for step in range(chips):
            head = chip ^ step
            own_s[head] = own[step][...]
            other_s[head] = other[step][...]
        rows = whole_ref.shape[0]

        def upright(ref):
            return ref[...].reshape(chips * HEAD_DIM, rows).astype(jnp.float32).T.astype(jnp.bfloat16)

        middle = (
            whole_ref[...]
            + jnp.dot(upright(own_s), wo_ref[...], preferred_element_type=jnp.float32)
            + jnp.dot(upright(other_s), wx_ref[...], preferred_element_type=jnp.float32)
        )
        middle_s[...] = middle
        scale = lax.rsqrt(jnp.mean(middle * middle, axis=1, keepdims=True) + epsilon)
        post_s[...] = (middle * scale * gain_ref[...].astype(jnp.float32)).astype(jnp.bfloat16)
        sum_s[...] = jnp.zeros_like(sum_s)

    post = post_s[...]
    gate = jnp.dot(post, wg_ref[...], preferred_element_type=jnp.float32)
    up = jnp.dot(post, wu_ref[...], preferred_element_type=jnp.float32)
    hidden = (gate / (1.0 + jnp.exp(-gate)) * up).astype(jnp.bfloat16)
    sum_s[...] += jnp.dot(hidden, wd_ref[...], preferred_element_type=jnp.float32)

    @pl.when(index == steps - 1)
    def _():
        part = sum_s[...]
        kept = middle_s[...] + part
        if last:
            cut = part.shape[1] // 2
            sent_ref[...] = jnp.where(side == 0, part[:, cut:], part[:, :cut]).astype(jnp.bfloat16)
            kept_ref[...] = jnp.where(side == 0, kept[:, :cut], kept[:, cut:])
        else:
            sent_ref[...] = part.astype(jnp.bfloat16)
            kept_ref[...] = kept


HIDDEN = 256


def feed(last, chips, layer, place, whole, gain, wo, wx, wg, wu, wd, own, other):
    rows, width = whole.shape
    mine = wg.shape[2]
    steps = mine // HIDDEN
    half = wo.shape[1]
    spec = lambda shape: pl.BlockSpec(shape, lambda i, p: (0,) * len(shape))
    out_width = width // 2 if last else width
    return pl.pallas_call(
        functools.partial(feed_kernel, last, chips, steps),
        grid_spec=pltpu.PrefetchScalarGridSpec(
            num_scalar_prefetch=1,
            grid=(steps,),
            in_specs=[
                spec((rows, width)),
                spec((1, width)),
                pl.BlockSpec((None, half, width), lambda i, p: (layer, 0, 0)),
                spec((half, width)),
                pl.BlockSpec((None, width, HIDDEN), lambda i, p: (layer, 0, i)),
                pl.BlockSpec((None, width, HIDDEN), lambda i, p: (layer, 0, i)),
                pl.BlockSpec((None, HIDDEN, width), lambda i, p: (layer, i, 0)),
            ]
            + [spec((HEAD_DIM, rows))] * (2 * chips),
            out_specs=[spec((rows, out_width))] * 2,
            scratch_shapes=[
                pltpu.VMEM((rows, width), jnp.float32),
                pltpu.VMEM((rows, width), jnp.bfloat16),
                pltpu.VMEM((rows, width), jnp.float32),
                pltpu.VMEM((chips, HEAD_DIM, rows), jnp.bfloat16),
                pltpu.VMEM((chips, HEAD_DIM, rows), jnp.bfloat16),
            ],
        ),
        out_shape=[
            jax.ShapeDtypeStruct((rows, out_width), jnp.float32),
            jax.ShapeDtypeStruct((rows, out_width), jnp.bfloat16),
        ],
        compiler_params=pltpu.CompilerParams(vmem_limit_bytes=60 * 1024 * 1024),
        name="feed",
    )(place, whole, gain[layer][None], wo, wx, wg, wu, wd, *own, *other)


def by_chip(
    tokens,
    norm_before,
    query_weight,
    key_weight,
    value_weight,
    output_weight,
    norm_after,
    gate_weight,
    up_weight,
    down_weight,
    block_image,
    image_width,
):
    local_rows = tokens.shape[0]
    shard_blocks = local_rows // BLK
    columns = lax.axis_size("col")
    places = lax.axis_size("row") * columns
    chips = places // 2
    here = lax.axis_index(("row", "col"))
    side = lax.axis_index("tp")
    row, column = here // columns, here % columns
    chip, core = (row // 2) * columns + column, row % 2
    place = jnp.stack([chip, core, side]).astype(jnp.int32)

    def chip_swap(x, step):
        pairs = []
        for p in range(places):
            at, c = (p // columns // 2) * columns + p % columns, (p // columns) % 2
            to = at ^ step
            pairs.append((p, ((to // columns) * 2 + c) * columns + to % columns))
        return lax.ppermute(x, ("row", "col"), pairs)

    def core_swap(x):
        return lax.ppermute(
            x, ("row", "col"), [(p, (p // columns ^ 1) * columns + p % columns) for p in range(places)]
        )

    def side_swap(x):
        return lax.ppermute(x, "tp", [(0, 1), (1, 0)])

    other_tokens = side_swap(tokens)
    tables = block_tables(block_image, image_width)
    live = jnp.clip(tables[3] - tables[1], 0, BLK)
    table = jnp.stack([tables[0], tables[4], tables[5], live])
    cosine, sine = rope_transposed(tables, here * shard_blocks, shard_blocks)
    layer_count = query_weight.shape[0]
    a, b = tokens, other_tokens
    other_output = [side_swap(output_weight[layer]) for layer in range(layer_count)]
    for layer in range(layer_count):
        whole, pieces = project(
            layer == 0, chips, layer, place, a, b, norm_before,
            query_weight, key_weight, value_weight, cosine, sine,
        )
        own = [pieces[0]] + [chip_swap(pieces[step], step) for step in range(1, chips)]
        far = [core_swap(piece[1:]) for piece in own]
        results = attend(chips, columns, table, place, own, far)
        back = [results[0]] + [chip_swap(results[step], step) for step in range(1, chips)]
        across = [side_swap(piece) for piece in back]
        a, sent = feed(
            layer + 1 == layer_count, chips, layer, place, whole, norm_after,
            output_weight, other_output[layer], gate_weight, up_weight, down_weight, back, across,
        )
        b = side_swap(sent)
    return a + b.astype(jnp.float32)


def shifted(x, axis, by):
    size = lax.axis_size(axis)
    pairs = [(i, i + by) for i in range(size) if 0 <= i + by < size]
    return lax.ppermute(x, axis, pairs)


def plain_tables(block_image, image_width):
    block_total = block_image.shape[0]
    images = jnp.arange(image_width.shape[0], dtype=jnp.int32)
    member = (block_image[:, None] == images[None, :]).astype(jnp.int32)
    count = jnp.sum(member, axis=0)
    start = jnp.sum((block_image[:, None] < images[None, :]).astype(jnp.int32), axis=0)
    slots = count * BLK
    filled = slots // image_width * image_width
    first = jnp.sum(member * start[None, :], axis=1)
    offset = (jnp.arange(block_total, dtype=jnp.int32) - first) * BLK
    return (
        block_image,
        offset,
        jnp.sum(member * image_width[None, :], axis=1),
        jnp.sum(member * filled[None, :], axis=1),
    )


def token_rows(tables, first_block, shard_blocks):
    image, offset, width, filled = [
        jnp.repeat(lax.dynamic_slice_in_dim(table, first_block, shard_blocks), BLK)
        for table in tables
    ]
    slot = offset + jnp.arange(shard_blocks * BLK, dtype=jnp.int32) % BLK
    return (image, slot // width, slot % width, slot < filled)


def key_tags(tables, device, devices, shard_blocks):
    inside = (device >= 0) & (device < devices)
    safe = jnp.clip(device, 0, devices - 1)
    image, patch_row, patch_column, live = token_rows(tables, safe * shard_blocks, shard_blocks)
    return jnp.where(inside & live, image, -1)


def rope_tables(patch_row, patch_column):
    half = HEAD_DIM // 2
    frequency = theta ** (-2.0 * jnp.arange(half, dtype=jnp.float32) / HEAD_DIM)
    angle = jnp.concatenate(
        [
            patch_row.astype(jnp.float32)[:, None] * frequency[None, 0::2],
            patch_column.astype(jnp.float32)[:, None] * frequency[None, 1::2],
        ],
        axis=1,
    )
    return (jnp.cos(angle), jnp.sin(angle))


def rotate(heads, cosine, sine):
    half = heads.shape[-1] // 2
    front = heads[..., :half]
    back = heads[..., half:]
    cosine = cosine[:, None, :]
    sine = sine[:, None, :]
    return jnp.concatenate([front * cosine - back * sine, back * cosine + front * sine], axis=-1)


def normalize(values, gain):
    scale = lax.rsqrt(jnp.mean(values * values, axis=-1, keepdims=True) + epsilon)
    return (values * scale * gain.astype(jnp.float32)).astype(jnp.bfloat16)


def attend_plain(state, block, tags, query, query_image):
    best, total, summed = state
    rows = block.shape[0]
    heads = query.shape[1]
    depth = query.shape[2]
    keys = block[:, : heads * depth].reshape(rows, heads, depth)
    values = block[:, heads * depth :].reshape(rows, heads, depth)
    scores = jnp.einsum(
        "thd,uhd->thu", query, keys, preferred_element_type=jnp.float32
    ) * HEAD_DIM ** (-0.5)
    allowed = (query_image[:, None] == tags[None, :])[:, None, :]
    fresh = jnp.maximum(best, jnp.max(jnp.where(allowed, scores, masked), axis=-1))
    carry_scale = jnp.exp(best - fresh)
    raised = jnp.where(allowed, jnp.exp(scores - fresh[..., None]), 0.0)
    total = total * carry_scale + jnp.sum(raised, axis=-1)
    summed = summed * carry_scale[..., None] + jnp.einsum(
        "thu,uhd->thd", raised.astype(jnp.bfloat16), values, preferred_element_type=jnp.float32
    )
    return (fresh, total, summed)


def by_reach(
    tokens,
    norm_before,
    query_weight,
    key_weight,
    value_weight,
    output_weight,
    norm_after,
    gate_weight,
    up_weight,
    down_weight,
    block_image,
    image_width,
):
    local_rows = tokens.shape[0]
    shard_blocks = local_rows // BLK
    reach = SPAN // shard_blocks - 1
    devices = lax.axis_size(("row", "col"))
    place = lax.axis_index(("row", "col"))
    tables = plain_tables(block_image, image_width)
    own_image, patch_row, patch_column, own_live = token_rows(
        tables, place * shard_blocks, shard_blocks
    )
    own_tags = jnp.where(own_live, own_image, -1)
    cosine, sine = rope_tables(patch_row, patch_column)
    whole = lax.all_gather(tokens, "tp", axis=1, tiled=True).astype(jnp.float32)
    layer_input = tokens.astype(jnp.float32)
    layer_count = query_weight.shape[0]
    for layer in range(layer_count):
        normed = normalize(whole, norm_before[layer])
        query = jnp.dot(normed, query_weight[layer], preferred_element_type=jnp.float32)
        heads_here = query.shape[1] // HEAD_DIM
        query = rotate(query.reshape(local_rows, heads_here, HEAD_DIM), cosine, sine).astype(
            jnp.bfloat16
        )
        keys = jnp.dot(normed, key_weight[layer], preferred_element_type=jnp.float32)
        keys = rotate(keys.reshape(local_rows, heads_here, HEAD_DIM), cosine, sine).astype(
            jnp.bfloat16
        )
        values = jnp.dot(normed, value_weight[layer], preferred_element_type=jnp.float32).astype(
            jnp.bfloat16
        )
        pair = jnp.concatenate([keys.reshape(local_rows, heads_here * HEAD_DIM), values], axis=1)
        start_state = (
            jnp.full((local_rows, heads_here), masked, jnp.float32),
            jnp.zeros((local_rows, heads_here), jnp.float32),
            jnp.zeros((local_rows, heads_here, HEAD_DIM), jnp.float32),
        )
        state = attend_plain(start_state, pair, own_tags, query, own_image)
        lower = pair[None]
        upper = pair[None]
        stride = 1
        while stride <= reach:
            lower = jnp.concatenate([lower, shifted(lower, ("row", "col"), stride)], axis=0)
            upper = jnp.concatenate([upper, shifted(upper, ("row", "col"), -stride)], axis=0)
            stride = stride * 2

        def visit(inner, items):
            below, above, distance = items
            tags = jnp.concatenate(
                [
                    key_tags(tables, place - distance, devices, shard_blocks),
                    key_tags(tables, place + distance, devices, shard_blocks),
                ]
            )
            return (
                attend_plain(inner, jnp.concatenate([below, above], axis=0), tags, query, own_image),
                None,
            )

        state, unused = lax.scan(
            visit,
            state,
            (lower[1 : reach + 1], upper[1 : reach + 1], jnp.arange(1, reach + 1, dtype=jnp.int32)),
        )
        best, total, summed = state
        attended = (
            (summed / total[..., None])
            .reshape(local_rows, heads_here * HEAD_DIM)
            .astype(jnp.bfloat16)
        )
        mixed_part = jnp.dot(attended, output_weight[layer], preferred_element_type=jnp.float32)
        middle_own = layer_input + lax.psum_scatter(
            mixed_part, "tp", scatter_dimension=1, tiled=True
        )
        middle = lax.all_gather(middle_own, "tp", axis=1, tiled=True)
        post = normalize(middle, norm_after[layer])
        gate = jnp.dot(post, gate_weight[layer], preferred_element_type=jnp.float32)
        up = jnp.dot(post, up_weight[layer], preferred_element_type=jnp.float32)
        hidden = (jax.nn.silu(gate) * up).astype(jnp.bfloat16)
        down_part = jnp.dot(hidden, down_weight[layer], preferred_element_type=jnp.float32)
        layer_input = middle_own + lax.psum_scatter(
            down_part, "tp", scatter_dimension=1, tiled=True
        )
        if layer + 1 < layer_count:
            whole = lax.all_gather(layer_input, "tp", axis=1, tiled=True)
    return layer_input


def solution(mesh):
    placed = (
        P(("row", "col"), "tp"),
        P(),
        P(None, None, "tp"),
        P(None, None, "tp"),
        P(None, None, "tp"),
        P(None, "tp", None),
        P(),
        P(None, None, "tp"),
        P(None, None, "tp"),
        P(None, "tp", None),
        P(),
        P(),
    )
    rows, columns, sides = mesh.shape["row"], mesh.shape["col"], mesh.shape["tp"]
    chips = rows * columns // 2

    def run(*arrays):
        tokens, query_weight = arrays[0], arrays[2]
        heads = query_weight.shape[2] // HEAD_DIM
        fits = (
            sides == 2
            and rows % 2 == 0
            and heads == chips * sides
            and chips & (chips - 1) == 0
            and arrays[11].shape[0] <= HEAD_DIM
            and tokens.shape[0] % (rows * columns * TILE) == 0
        )
        return jax.shard_map(
            by_chip if fits else by_reach,
            mesh=mesh,
            in_specs=placed,
            out_specs=P(("row", "col"), "tp"),
            check_vma=False,
        )(*arrays)

    return run
```
